32 devices in a mesh: dp: 2 (over x), vocab: 16 (over z, y, core).
Axes of the slice: x: 2, y: 2, z: 4, core: 2. Of those that a mesh axis runs over, the one named last changes fastest.
Arguments:
- pooled_grad: bfloat16 [1024, 1024], P(('dp', 'vocab')), may hold values from -12 to 12
- token_ids: int32 [1024, 16], P(('dp', 'vocab')), may hold values from 0 to 8191, as said below
Outputs:
- table_grad: float32 [8192, 1024], P(('dp', 'vocab'))
The draws below stay inside these ranges and needn't reach their ends.
Inputs may be any that keep to these rules, and one draw needn't show every extreme that they name: `token_ids`: the owner of id r is (r // 256) % 16. Among the ids of one device's 32 positions at most 96 have the same owner; in every group of 16 devices along vocab some owner gets exactly 96 ids from each of them.
All inputs are finite; a program needn't handle non-finite values.
Results may differ from the reference program's by a relative error of at most 0.0075.
Values may be sent and summed in bfloat16 or wider, within the bound.
No kernel may reach another device: no remote copies, remote signals or barrier semaphores. Data moves between devices by JAX's collectives and lax.ppermute only.
A program may use at most 64 MiB of HBM per device.

```python
import jax
import jax.numpy as jnp
from jax import lax

D = 1024
ROWS_DEV = 256
POS_DEV = 32
LIST = 16
GROUPS = 2
OWNERS = 16
CAPACITY = 96
POSITIONS = 1024
VOCAB = 8192
COLUMN_ROWS = 512


def draw_token_ids(key, part):
    entries = POS_DEV * LIST
    slots_all = OWNERS * CAPACITY
    cand_owner = jnp.arange(slots_all, dtype=jnp.int32) // CAPACITY

    def group_levels(group_key):
        level_key, hot_key = jax.random.split(group_key)
        levels = jax.random.randint(level_key, (OWNERS,), 0, 4, dtype=jnp.int32)
        hottest = jax.random.randint(hot_key, (), 0, OWNERS, dtype=jnp.int32)
        return jnp.where(jnp.arange(OWNERS, dtype=jnp.int32) == hottest, 8, levels)
    group_keys = jax.random.split(jax.random.fold_in(key, 17), GROUPS)
    all_levels = jax.vmap(group_levels)(group_keys)
    device_keys = jax.random.split(jax.random.fold_in(key, 29), GROUPS * OWNERS)

    def device_ids(device_key, levels):
        pick_key, order_key, outer_key, inner_key = jax.random.split(device_key, 4)
        noise = jax.random.randint(pick_key, (slots_all,), 0, 4096, dtype=jnp.int32)
        scores = (levels[cand_owner] * 4096 + noise) * slots_all + jnp.arange(slots_all, dtype=jnp.int32)
        _, chosen = lax.top_k(scores, entries)
        owner_list = cand_owner[chosen]
        owner_list = owner_list[jax.random.permutation(order_key, entries)]
        outer = jax.random.randint(outer_key, (entries,), 0, COLUMN_ROWS, dtype=jnp.int32)
        inner = jax.random.randint(inner_key, (entries,), 0, outer + 1, dtype=jnp.int32)
        return (inner // ROWS_DEV * OWNERS + owner_list) * ROWS_DEV + inner % ROWS_DEV
    device_levels = jnp.repeat(all_levels, OWNERS, axis=0)
    flat_ids = jax.vmap(device_ids)(device_keys, device_levels)
    return flat_ids.reshape(POSITIONS, LIST)


def steps_of(rng, extent, pieces, least, top_value):
    def one(dim, shards_of):
        draws = jax.random.uniform(jax.random.fold_in(jax.random.fold_in(rng, 6), dim), (shards_of,), jnp.float32, least / len(pieces), top_value / len(pieces))
        return jnp.repeat(jnp.exp(draws), extent[dim] // shards_of).reshape((-1,) + (1,) * (len(extent) - dim - 1))

    factor_of = one(*pieces[0])
    for cut in pieces[1:]:
        factor_of = factor_of * one(*cut)
    return factor_of


def gaussian(rng, extent, spread, bound, cuts=(), kind=jnp.bfloat16):
    result = spread * jax.random.normal(rng, extent, jnp.float32)
    if cuts:
        result = result * steps_of(rng, extent, cuts, -0.22, 0.18)
    return jnp.clip(result, -bound, bound).astype(kind)


def setup_inputs(seed: int = 0) -> dict:
    splits = jax.random.split(jax.random.key(seed), 3)
    pooled_grad = gaussian(splits[0], (POSITIONS, D), 2.0, 12.0, ((0, 32),))
    token_ids = draw_token_ids(jax.random.fold_in(splits[2], 71), 0)
    return dict(pooled_grad=pooled_grad, token_ids=token_ids)


def reference(pooled_grad, token_ids):
    id_share = (pooled_grad.astype(jnp.float32) / LIST).astype(jnp.bfloat16)
    width = pooled_grad.shape[1]
    grouped_share = id_share.reshape(GROUPS, -1, width)
    grouped_ids = token_ids.reshape(GROUPS, -1, LIST)

    def add_group(running, inputs):
        shares, id_lists = inputs
        copies = jnp.repeat(shares.astype(jnp.float32), LIST, axis=0)
        partial_value = jax.ops.segment_sum(copies, id_lists.reshape(-1).astype(jnp.int32), num_segments=VOCAB)
        rounded = lax.optimization_barrier(partial_value.astype(jnp.bfloat16))
        return running + rounded.astype(jnp.float32), None

    table_grad, _ = lax.scan(add_group, jnp.zeros((VOCAB, width), jnp.float32), (grouped_share, grouped_ids))
    return table_grad
```

```python
import functools

import jax
import jax.numpy as jnp
from jax import lax
from jax.experimental import pallas as pl
from jax.experimental.pallas import tpu as pltpu
from jax.sharding import PartitionSpec as P


ROWS_DEV = 256
AXES = ("dp", "vocab")
SUB = 8
LANES = 128
RADIX = 256


def log2(n):
    bits = n.bit_length() - 1
    assert n == 1 << bits
    return bits


def pack_kernel(grad_ref, ids_ref, msg_ref):
    places, positions = ids_ref.shape
    width = grad_ref.shape[1]
    blocks = positions // SUB
    step = 2 * places
    ids = ids_ref[...]
    digits = jnp.concatenate([ids & (RADIX - 1), (ids >> log2(RADIX)) - RADIX], axis=0)
    lane = lax.broadcasted_iota(jnp.int32, (step, LANES), 1)
    digit = lax.broadcasted_iota(jnp.int32, (step, LANES), 0)
    spread = (lane % step == digit).astype(jnp.bfloat16)
    by_position = lax.dot_general(
        digits.astype(jnp.float32).astype(jnp.bfloat16), spread, (((0,), (0,)), ((), ())),
        preferred_element_type=jnp.float32,
    )
    lane = lax.broadcasted_iota(jnp.int32, (SUB, LANES), 1)
    tile = jnp.zeros((SUB, LANES), jnp.float32)
    for b in range(blocks):
        tile = jnp.where(lane // step == b, by_position[b * SUB:(b + 1) * SUB], tile)
        msg_ref[:, b * width:(b + 1) * width] = grad_ref[b * SUB:(b + 1) * SUB, :]
    msg_ref[:, blocks * width:] = tile.astype(jnp.bfloat16)


def group_sum(refs, runs, blocks, places, width, first_row):
    step = 2 * places
    digits, rows = [], []
    for ref, (lo, hi) in [(ref, run) for run in runs for ref in refs]:
        digits.append(ref[lo:hi, blocks * width:])
    digits = jnp.concatenate(digits, axis=0)
    lane = lax.broadcasted_iota(jnp.int32, digits.shape, 1)
    per_block = []
    for b in range(blocks):
        per_block.append(jnp.where(lane // step == b, digits, jnp.zeros_like(digits)))
        for ref, (lo, hi) in [(ref, run) for run in runs for ref in refs]:
            rows.append(ref[lo:hi, b * width:(b + 1) * width])
    per_block = jnp.concatenate(per_block, axis=0)
    rows = jnp.concatenate(rows, axis=0)
    lane = lax.broadcasted_iota(jnp.int32, (places, LANES), 1)
    place = lax.broadcasted_iota(jnp.int32, (places, LANES), 0)
    weight = jnp.where(lane % step == place, 1.0, 0.0)
    weight = jnp.where(lane % step == place + places, float(RADIX), weight)
    ids = lax.dot_general(
        weight.astype(jnp.bfloat16), per_block, (((1,), (1,)), ((), ())),
        preferred_element_type=jnp.float32,
    )
    local = ids + float(RADIX * RADIX) - first_row.astype(jnp.float32)
    local = jnp.where((local >= 0.0) & (local < float(ROWS_DEV)), local, -1.0).astype(jnp.bfloat16)
    shape = (ROWS_DEV, local.shape[1])
    wanted = lax.broadcasted_iota(jnp.int32, shape, 0).astype(jnp.float32).astype(jnp.bfloat16)
    share = jnp.bfloat16(1.0 / places)
    counts = jnp.zeros(shape, jnp.bfloat16)
    for j in range(places):
        hit = wanted == jnp.broadcast_to(local[j:j + 1, :], shape)
        counts = counts + jnp.where(hit, share, jnp.bfloat16(0))
    return jnp.dot(counts, rows, preferred_element_type=jnp.float32)


def early_kernel(row_ref, own_ref, other_ref, acc_ref, *, group_runs, blocks, places, width):
    for g, runs in enumerate(group_runs):
        acc_ref[g] = group_sum((own_ref, other_ref), runs, blocks, places, width, row_ref[0])


def late_kernel(row_ref, own_ref, other_ref, acc_ref, out_ref, *, group_runs, blocks, places, width):
    total = None
    for g, runs in enumerate(group_runs):
        part = acc_ref[g] + group_sum((own_ref, other_ref), runs, blocks, places, width, row_ref[0])
        part = part.astype(jnp.bfloat16).astype(jnp.float32)
        total = part if total is None else total + part
    out_ref[...] = total


def runs_of(keys, group):
    runs = []
    for k, key in enumerate(keys):
        if key != group:
            continue
        if runs and runs[-1][1] == k * SUB:
            runs[-1] = (runs[-1][0], (k + 1) * SUB)
        else:
            runs.append((k * SUB, (k + 1) * SUB))
    return runs


def local(pooled_grad, token_ids, *, groups, owners):
    devices = groups * owners
    bits = log2(devices)
    positions, width = pooled_grad.shape
    places = token_ids.shape[1]
    blocks = positions // SUB
    assert blocks * 2 * places <= LANES
    vmem = pl.BlockSpec(memory_space=pltpu.VMEM)
    smem = pl.BlockSpec(memory_space=pltpu.SMEM)

    def move(x, flip):
        return lax.ppermute(x, AXES, [(d, d ^ flip) for d in range(devices)])

    def join(*parts):
        return jnp.concatenate(parts, axis=0)

    message = pl.pallas_call(
        pack_kernel,
        out_shape=jax.ShapeDtypeStruct((SUB, blocks * width + LANES), jnp.bfloat16),
        in_specs=[vmem, vmem],
        out_specs=vmem,
    )(pooled_grad, token_ids.T)

    core, near, far = 1, 2, 1 << (bits - 1)
    others = [1 << b for b in range(2, bits - 1)]
    keys = [0]
    while len(others) > 2:
        bit = others.pop()
        message = join(message, move(message, bit))
        keys = keys + [k ^ bit for k in keys]
    one, two = others
    got = {flip: move(message, flip) for flip in (one, two, one ^ two)}
    got[0] = message

    def spread(flips):
        source = join(*[got[f] for f in flips])
        source_keys = [k ^ f for f in flips for k in keys]
        pieces, piece_keys = [source], list(source_keys)
        for flip in (far, near, far | near):
            pieces.append(move(source, flip))
            piece_keys += [k ^ flip for k in source_keys]
        own = join(*pieces)
        return own, move(own, core), piece_keys

    first_row = ((lax.axis_index("dp") * owners + lax.axis_index("vocab")) * ROWS_DEV).astype(jnp.int32).reshape(1)
    early_own, early_other, early_keys = spread((0, one))
    late_own, late_other, late_keys = spread((two, one ^ two))

    def group_runs(piece_keys):
        piece_groups = [k // owners for k in piece_keys]
        return [runs_of(piece_groups, g) for g in range(groups)]

    shape = dict(blocks=blocks, places=places, width=width)
    acc = pl.pallas_call(
        functools.partial(early_kernel, group_runs=group_runs(early_keys), **shape),
        out_shape=jax.ShapeDtypeStruct((groups, ROWS_DEV, width), jnp.float32),
        in_specs=[smem, vmem, vmem],
        out_specs=vmem,
    )(first_row, early_own, early_other)
    return pl.pallas_call(
        functools.partial(late_kernel, group_runs=group_runs(late_keys), **shape),
        out_shape=jax.ShapeDtypeStruct((ROWS_DEV, width), jnp.float32),
        in_specs=[smem, vmem, vmem, vmem],
        out_specs=vmem,
    )(first_row, late_own, late_other, acc)


def solution(mesh):
    groups, owners = mesh.shape["dp"], mesh.shape["vocab"]

    def body(pooled_grad, token_ids):
        return local(pooled_grad, token_ids, groups=groups, owners=owners)

    in_specs = (P(AXES, None), P(AXES, None))
    out_specs = P(AXES, None)
    return jax.shard_map(body, mesh=mesh, in_specs=in_specs, out_specs=out_specs, check_vma=False)
```

```python
import functools

import jax
import jax.numpy as jnp
from jax import lax
from jax.experimental import pallas as pl
from jax.experimental.pallas import tpu as pltpu
from jax.sharding import PartitionSpec as P


ROWS_DEV = 256
AXES = ("dp", "vocab")
SUB = 8
LANES = 128
RADIX = 256

CHUNKS = 4


def log2(n):
    bits = n.bit_length() - 1
    assert n == 1 << bits
    return bits


def pack_kernel(grad_hbm, ids_hbm, msg_ref, ids_ref, grad_sem, ids_sem):
    places, positions = ids_ref.shape
    width = grad_hbm.shape[1]
    blocks = positions // SUB
    step = 2 * places
    ids_copy = pltpu.make_async_copy(ids_hbm, ids_ref, ids_sem)
    ids_copy.start()
    grad_copies = []
    for b in range(blocks):
        copy = pltpu.make_async_copy(
            grad_hbm.at[b * SUB:(b + 1) * SUB, :], msg_ref.at[:, b * width:(b + 1) * width], grad_sem.at[b]
        )
        copy.start()
        grad_copies.append(copy)
    ids_copy.wait()
    ids = ids_ref[...]
    digits = jnp.concatenate([ids & (RADIX - 1), (ids >> log2(RADIX)) - RADIX], axis=0)
    lane = lax.broadcasted_iota(jnp.int32, (step, LANES), 1)
    digit = lax.broadcasted_iota(jnp.int32, (step, LANES), 0)
    spread = (lane % step == digit).astype(jnp.bfloat16)
    by_position = lax.dot_general(
        digits.astype(jnp.float32).astype(jnp.bfloat16), spread, (((0,), (0,)), ((), ())),
        preferred_element_type=jnp.float32,
    )
    lane = lax.broadcasted_iota(jnp.int32, (SUB, LANES), 1)
    tile = jnp.zeros((SUB, LANES), jnp.float32)
    for b in range(blocks):
        tile = jnp.where(lane // step == b, by_position[b * SUB:(b + 1) * SUB], tile)
    msg_ref[:, blocks * width:] = tile.astype(jnp.bfloat16)
    for copy in grad_copies:
        copy.wait()


def pieces_of(refs, group_runs, group):
    return [(ref, run) for ref, runs in zip(refs, group_runs) for run in runs[group]]


def counts_of(pieces, blocks, places, width, first_row):
    step = 2 * places
    digits = jnp.concatenate([ref[lo:hi, blocks * width:] for ref, (lo, hi) in pieces], axis=0)
    lane = lax.broadcasted_iota(jnp.int32, digits.shape, 1)
    per_block = jnp.concatenate(
        [jnp.where(lane // step == b, digits, jnp.zeros_like(digits)) for b in range(blocks)], axis=0
    )
    lane = lax.broadcasted_iota(jnp.int32, (places, LANES), 1)
    place = lax.broadcasted_iota(jnp.int32, (places, LANES), 0)
    weight = jnp.where(lane % step == place, 1.0, 0.0)
    weight = jnp.where(lane % step == place + places, float(RADIX), weight)
    ids = lax.dot_general(
        weight.astype(jnp.bfloat16), per_block, (((1,), (1,)), ((), ())),
        preferred_element_type=jnp.float32,
    )
    local = ids + float(RADIX * RADIX) - first_row.astype(jnp.float32)
    local = jnp.where((local >= 0.0) & (local < float(ROWS_DEV)), local, -1.0).astype(jnp.bfloat16)
    shape = (ROWS_DEV, local.shape[1])
    wanted = lax.broadcasted_iota(jnp.int32, shape, 0).astype(jnp.float32).astype(jnp.bfloat16)
    share = jnp.bfloat16(1.0 / places)
    counts = jnp.zeros(shape, jnp.bfloat16)
    for j in range(places):
        hit = wanted == jnp.broadcast_to(local[j:j + 1, :], shape)
        counts = counts + jnp.where(hit, share, jnp.bfloat16(0))
    return counts


def rows_of(pieces, blocks, width, lo_col, hi_col):
    return jnp.concatenate(
        [ref[lo:hi, b * width + lo_col:b * width + hi_col] for b in range(blocks) for ref, (lo, hi) in pieces], axis=0
    )


def gather_kernel(row_ref, *refs, group_runs, blocks, places, width, add):
    acc_ref = refs[-1]
    pieces_refs = refs[:len(group_runs)]
    for g in range(acc_ref.shape[0]):
        pieces = pieces_of(pieces_refs, group_runs, g)
        counts = counts_of(pieces, blocks, places, width, row_ref[0])
        part = jnp.dot(counts, rows_of(pieces, blocks, width, 0, width), preferred_element_type=jnp.float32)
        acc_ref[g] = refs[len(group_runs)][g] + part if add else part


def last_kernel(row_ref, *refs, group_runs, blocks, places, width, chunk):
    acc_ref, out_hbm, out_ref, out_sem = refs[len(group_runs):]
    pieces_refs = refs[:len(group_runs)]
    groups = acc_ref.shape[0]
    pieces = [pieces_of(pieces_refs, group_runs, g) for g in range(groups)]
    counts = [counts_of(p, blocks, places, width, row_ref[0]) for p in pieces]
    copies = []
    for c, lo in enumerate(range(0, width, chunk)):
        hi = lo + chunk
        total = None
        for g in range(groups):
            rows = rows_of(pieces[g], blocks, width, lo, hi)
            part = acc_ref[g, :, lo:hi] + jnp.dot(counts[g], rows, preferred_element_type=jnp.float32)
            part = part.astype(jnp.bfloat16).astype(jnp.float32)
            total = part if total is None else total + part
        out_ref[:, lo:hi] = total
        copy = pltpu.make_async_copy(out_ref.at[:, lo:hi], out_hbm.at[:, lo:hi], out_sem.at[c])
        copy.start()
        copies.append(copy)
    for copy in copies:
        copy.wait()


def runs_of(keys, group):
    runs = []
    for k, key in enumerate(keys):
        if key != group:
            continue
        if runs and runs[-1][1] == k * SUB:
            runs[-1] = (runs[-1][0], (k + 1) * SUB)
        else:
            runs.append((k * SUB, (k + 1) * SUB))
    return runs


def local(pooled_grad, token_ids, *, groups, owners):
    devices = groups * owners
    bits = log2(devices)
    positions, width = pooled_grad.shape
    places = token_ids.shape[1]
    blocks = positions // SUB
    assert blocks * 2 * places <= LANES
    vmem = pl.BlockSpec(memory_space=pltpu.VMEM)
    smem = pl.BlockSpec(memory_space=pltpu.SMEM)
    hbm = pl.BlockSpec(memory_space=pltpu.HBM)

    def move(x, flip):
        return lax.ppermute(x, AXES, [(d, d ^ flip) for d in range(devices)])

    def join(*parts):
        return jnp.concatenate(parts, axis=0)

    message = pl.pallas_call(
        pack_kernel,
        out_shape=jax.ShapeDtypeStruct((SUB, blocks * width + LANES), jnp.bfloat16),
        in_specs=[hbm, hbm],
        out_specs=vmem,
        scratch_shapes=[
            pltpu.VMEM((places, positions), jnp.int32),
            pltpu.SemaphoreType.DMA((blocks,)),
            pltpu.SemaphoreType.DMA,
        ],
        compiler_params=pltpu.CompilerParams(vmem_limit_bytes=8 << 20),
    )(pltpu.with_memory_space_constraint(pooled_grad, pltpu.HBM), pltpu.with_memory_space_constraint(token_ids.T, pltpu.HBM))

    core, near, far = 1, 2, 1 << (bits - 1)
    others = [1 << b for b in range(2, bits - 1)]
    keys = [0]
    while len(others) > 2:
        bit = others.pop()
        message = join(message, move(message, bit))
        keys = keys + [k ^ bit for k in keys]
    one, two = others
    got = {flip: move(message, flip) for flip in (one, two, one ^ two)}
    got[0] = message

    def spread(flips):
        source = join(*[got[f] for f in flips])
        keys_of = [[k ^ f ^ flip for f in flips for k in keys] for flip in (0, far, near, far | near)]
        pieces = [source] + [move(source, flip) for flip in (far, near, far | near)]
        return pieces, keys_of

    def runs(keys_of):
        groups_of = [k // owners for ks in keys_of for k in ks]
        return [runs_of(groups_of, g) for g in range(groups)]

    first_row = ((lax.axis_index("dp") * owners + lax.axis_index("vocab")) * ROWS_DEV).astype(jnp.int32).reshape(1)
    shape = dict(blocks=blocks, places=places, width=width)

    def limit(arrays):
        held = sum(x.nbytes for x in arrays) + groups * ROWS_DEV * width * 4
        return pltpu.CompilerParams(vmem_limit_bytes=min((8 << 20) + 3 * held, 60 << 20))

    def gather(arrays, keys_list, acc=None):
        kernel = functools.partial(gather_kernel, group_runs=[runs(k) for k in keys_list], add=acc is not None, **shape)
        args = (first_row, *arrays) if acc is None else (first_row, *arrays, acc)
        return pl.pallas_call(
            kernel,
            out_shape=jax.ShapeDtypeStruct((groups, ROWS_DEV, width), jnp.float32),
            in_specs=[smem] + [vmem] * (len(args) - 1),
            out_specs=vmem,
            input_output_aliases={} if acc is None else {len(args) - 1: 0},
            compiler_params=limit(args[1:]),
        )(*args)

    a_pieces, a_keys = spread((0, one))
    b_pieces, b_keys = spread((two, one ^ two))
    a_keys = sum(a_keys, [])
    a_own = join(*a_pieces)
    a_other = move(a_own, core)
    b_own = [join(*b_pieces[:2]), join(*b_pieces[2:])]
    b_keys = [b_keys[0] + b_keys[1], b_keys[2] + b_keys[3]]
    b_other = [move(b_own[0], core), move(b_own[1], core)]
    acc = gather((a_own, a_other), ([a_keys], [a_keys]))
    acc = gather((*b_own, b_other[0]), ([b_keys[0]], [b_keys[1]], [b_keys[0]]), acc)
    chunk = width // CHUNKS
    return pl.pallas_call(
        functools.partial(last_kernel, group_runs=[runs([b_keys[1]])], chunk=chunk, **shape),
        out_shape=jax.ShapeDtypeStruct((ROWS_DEV, width), jnp.float32),
        in_specs=[smem, vmem, vmem],
        out_specs=hbm,
        scratch_shapes=[pltpu.VMEM((ROWS_DEV, width), jnp.float32), pltpu.SemaphoreType.DMA((CHUNKS,))],
        compiler_params=limit([b_other[1], acc]),
    )(first_row, b_other[1], acc)


def solution(mesh):
    groups, owners = mesh.shape["dp"], mesh.shape["vocab"]

    def body(pooled_grad, token_ids):
        return local(pooled_grad, token_ids, groups=groups, owners=owners)

    in_specs = (P(AXES, None), P(AXES, None))
    out_specs = P(AXES, None)
    return jax.shard_map(body, mesh=mesh, in_specs=in_specs, out_specs=out_specs, check_vma=False)
```

```python
import functools

import jax
import jax.numpy as jnp
from jax import lax
from jax.experimental import pallas as pl
from jax.experimental.pallas import tpu as pltpu
from jax.sharding import PartitionSpec as P


ROWS_DEV = 256
AXES = ("dp", "vocab")
SUB = 8
LANES = 128
RADIX = 256

CHUNKS = 4


def log2(n):
    bits = n.bit_length() - 1
    assert n == 1 << bits
    return bits


def pack_kernel(grad_hbm, ids_hbm, msg_ref, ids_ref, grad_sem, ids_sem):
    places, positions = ids_ref.shape
    width = grad_hbm.shape[1]
    blocks = positions // SUB
    step = 2 * places
    ids_copy = pltpu.make_async_copy(ids_hbm, ids_ref, ids_sem)
    ids_copy.start()
    grad_copies = []
    for b in range(blocks):
        copy = pltpu.make_async_copy(
            grad_hbm.at[b * SUB:(b + 1) * SUB, :], msg_ref.at[:, b * width:(b + 1) * width], grad_sem.at[b]
        )
        copy.start()
        grad_copies.append(copy)
    ids_copy.wait()
    ids = ids_ref[...]
    digits = jnp.concatenate([ids & (RADIX - 1), (ids >> log2(RADIX)) - RADIX], axis=0)
    lane = lax.broadcasted_iota(jnp.int32, (step, LANES), 1)
    digit = lax.broadcasted_iota(jnp.int32, (step, LANES), 0)
    spread = (lane % step == digit).astype(jnp.bfloat16)
    by_position = lax.dot_general(
        digits.astype(jnp.float32).astype(jnp.bfloat16), spread, (((0,), (0,)), ((), ())),
        preferred_element_type=jnp.float32,
    )
    lane = lax.broadcasted_iota(jnp.int32, (SUB, LANES), 1)
    tile = jnp.zeros((SUB, LANES), jnp.float32)
    for b in range(blocks):
        tile = jnp.where(lane // step == b, by_position[b * SUB:(b + 1) * SUB], tile)
    msg_ref[:, blocks * width:] = tile.astype(jnp.bfloat16)
    for copy in grad_copies:
        copy.wait()


def pieces_of(refs, group_runs, group):
    return [(ref, run) for ref, runs in zip(refs, group_runs) for run in runs[group]]


def counts_of(pieces, blocks, places, width, first_row):
    step = 2 * places
    digits = jnp.concatenate([ref[lo:hi, blocks * width:] for ref, (lo, hi) in pieces], axis=0)
    lane = lax.broadcasted_iota(jnp.int32, digits.shape, 1)
    per_block = jnp.concatenate(
        [jnp.where(lane // step == b, digits, jnp.zeros_like(digits)) for b in range(blocks)], axis=0
    )
    lane = lax.broadcasted_iota(jnp.int32, (places, LANES), 1)
    place = lax.broadcasted_iota(jnp.int32, (places, LANES), 0)
    weight = jnp.where(lane % step == place, 1.0, 0.0)
    weight = jnp.where(lane % step == place + places, float(RADIX), weight)
    ids = lax.dot_general(
        weight.astype(jnp.bfloat16), per_block, (((1,), (1,)), ((), ())),
        preferred_element_type=jnp.float32,
    )
    local = ids + float(RADIX * RADIX) - first_row.astype(jnp.float32)
    local = jnp.where((local >= 0.0) & (local < float(ROWS_DEV)), local, -1.0).astype(jnp.bfloat16)
    shape = (ROWS_DEV, local.shape[1])
    wanted = lax.broadcasted_iota(jnp.int32, shape, 0).astype(jnp.float32).astype(jnp.bfloat16)
    share = jnp.bfloat16(1.0 / places)
    counts = jnp.zeros(shape, jnp.bfloat16)
    for j in range(places):
        hit = wanted == jnp.broadcast_to(local[j:j + 1, :], shape)
        counts = counts + jnp.where(hit, share, jnp.bfloat16(0))
    return counts


def rows_of(pieces, blocks, width, lo_col, hi_col):
    return jnp.concatenate(
        [ref[lo:hi, b * width + lo_col:b * width + hi_col] for b in range(blocks) for ref, (lo, hi) in pieces], axis=0
    )


def gather_kernel(row_ref, *refs, group_runs, blocks, places, width, add):
    acc_ref = refs[-1]
    pieces_refs = refs[:len(group_runs)]
    for g in range(acc_ref.shape[0]):
        pieces = pieces_of(pieces_refs, group_runs, g)
        counts = counts_of(pieces, blocks, places, width, row_ref[0])
        part = jnp.dot(counts, rows_of(pieces, blocks, width, 0, width), preferred_element_type=jnp.float32)
        acc_ref[g] = refs[len(group_runs)][g] + part if add else part


def last_kernel(row_ref, *refs, group_runs, blocks, places, width, chunk):
    acc_ref, out_hbm, out_ref, out_sem = refs[len(group_runs):]
    pieces_refs = refs[:len(group_runs)]
    groups = acc_ref.shape[0]
    pieces = [pieces_of(pieces_refs, group_runs, g) for g in range(groups)]
    counts = [counts_of(p, blocks, places, width, row_ref[0]) for p in pieces]
    copies = []
    for c, lo in enumerate(range(0, width, chunk)):
        hi = lo + chunk
        total = None
        for g in range(groups):
            rows = rows_of(pieces[g], blocks, width, lo, hi)
            part = acc_ref[g, :, lo:hi] + jnp.dot(counts[g], rows, preferred_element_type=jnp.float32)
            part = part.astype(jnp.bfloat16).astype(jnp.float32)
            total = part if total is None else total + part
        out_ref[:, lo:hi] = total
        copy = pltpu.make_async_copy(out_ref.at[:, lo:hi], out_hbm.at[:, lo:hi], out_sem.at[c])
        copy.start()
        copies.append(copy)
    for copy in copies:
        copy.wait()


def runs_of(keys, group):
    runs = []
    for k, key in enumerate(keys):
        if key != group:
            continue
        if runs and runs[-1][1] == k * SUB:
            runs[-1] = (runs[-1][0], (k + 1) * SUB)
        else:
            runs.append((k * SUB, (k + 1) * SUB))
    return runs


def local(pooled_grad, token_ids, *, groups, owners):
    devices = groups * owners
    bits = log2(devices)
    positions, width = pooled_grad.shape
    places = token_ids.shape[1]
    blocks = positions // SUB
    assert blocks * 2 * places <= LANES
    vmem = pl.BlockSpec(memory_space=pltpu.VMEM)
    smem = pl.BlockSpec(memory_space=pltpu.SMEM)
    hbm = pl.BlockSpec(memory_space=pltpu.HBM)

    def move(x, flip):
        return lax.ppermute(x, AXES, [(d, d ^ flip) for d in range(devices)])

    def join(*parts):
        return jnp.concatenate(parts, axis=0)

    message = pl.pallas_call(
        pack_kernel,
        out_shape=jax.ShapeDtypeStruct((SUB, blocks * width + LANES), jnp.bfloat16),
        in_specs=[hbm, hbm],
        out_specs=vmem,
        scratch_shapes=[
            pltpu.VMEM((places, positions), jnp.int32),
            pltpu.SemaphoreType.DMA((blocks,)),
            pltpu.SemaphoreType.DMA,
        ],
        compiler_params=pltpu.CompilerParams(vmem_limit_bytes=8 << 20),
    )(pltpu.with_memory_space_constraint(pooled_grad, pltpu.HBM), pltpu.with_memory_space_constraint(token_ids.T, pltpu.HBM))

    core, near, far = 1, 2, 1 << (bits - 1)
    others = [1 << b for b in range(2, bits - 1)]
    keys = [0]
    while len(others) > 2:
        bit = others.pop()
        message = join(message, move(message, bit))
        keys = keys + [k ^ bit for k in keys]
    one, two = others
    moves = [
        ((0,), far | one), ((0,), far | near | two), ((0,), one | two),
        ((0, 1), near), ((0, 1), near | one), ((0, 1), far),
        ((2,), far), ((2, 3), one), ((2, 3), near), ((3,), far),
    ]
    held, held_keys = [message], [keys]
    for which, flip in moves:
        held.append(move(join(*[held[w] for w in which]), flip))
        held_keys.append([k ^ flip for w in which for k in held_keys[w]])

    def runs(keys_of):
        groups_of = [k // owners for k in keys_of]
        return [runs_of(groups_of, g) for g in range(groups)]

    def swap(which):
        own = join(*[held[w] for w in which])
        return own, move(own, core), sum([held_keys[w] for w in which], [])

    first_row = ((lax.axis_index("dp") * owners + lax.axis_index("vocab")) * ROWS_DEV).astype(jnp.int32).reshape(1)
    shape = dict(blocks=blocks, places=places, width=width)

    def limit(arrays):
        held = sum(x.nbytes for x in arrays) + groups * ROWS_DEV * width * 4
        return pltpu.CompilerParams(vmem_limit_bytes=min((8 << 20) + 3 * held, 60 << 20))

    def gather(arrays, keys_list, acc=None):
        kernel = functools.partial(gather_kernel, group_runs=[runs(k) for k in keys_list], add=acc is not None, **shape)
        args = (first_row, *arrays) if acc is None else (first_row, *arrays, acc)
        return pl.pallas_call(
            kernel,
            out_shape=jax.ShapeDtypeStruct((groups, ROWS_DEV, width), jnp.float32),
            in_specs=[smem] + [vmem] * (len(args) - 1),
            out_specs=vmem,
            input_output_aliases={} if acc is None else {len(args) - 1: 0},
            compiler_params=limit(args[1:]),
        )(*args)

    (most, most_other, most_keys), (some, some_other, some_keys), (late, late_other, late_keys) = [
        swap(which) for which in ((0, 1, 4, 5, 6), (2, 3, 7), (8, 9, 10))
    ]
    acc = gather((most, most_other), [most_keys, most_keys])
    acc = gather((some, some_other, late), [some_keys, some_keys, late_keys], acc)
    chunk = width // CHUNKS
    return pl.pallas_call(
        functools.partial(last_kernel, group_runs=[runs(late_keys)], chunk=chunk, **shape),
        out_shape=jax.ShapeDtypeStruct((ROWS_DEV, width), jnp.float32),
        in_specs=[smem, vmem, vmem],
        out_specs=hbm,
        scratch_shapes=[pltpu.VMEM((ROWS_DEV, width), jnp.float32), pltpu.SemaphoreType.DMA((CHUNKS,))],
        compiler_params=limit([late_other, acc]),
    )(first_row, late_other, acc)


def solution(mesh):
    groups, owners = mesh.shape["dp"], mesh.shape["vocab"]

    def body(pooled_grad, token_ids):
        return local(pooled_grad, token_ids, groups=groups, owners=owners)

    in_specs = (P(AXES, None), P(AXES, None))
    out_specs = P(AXES, None)
    return jax.shard_map(body, mesh=mesh, in_specs=in_specs, out_specs=out_specs, check_vma=False)
```
